256 devices in a mesh: groups: 2 (over y), freq: 128 (over z, x, core).
Axes of the slice: x: 4, y: 2, z: 16, core: 2. Of those that a mesh axis runs over, the one named last changes fastest.
The devices are a block of a 4x16x16 slice.
Arguments:
- primary_one: bfloat16 [1024, 512, 512], P(('groups', 'freq')), parts along dimension 0, may hold values from -6 to 6
- primary_two: bfloat16 [1024, 512, 512], P(('groups', 'freq')), parts along dimension 0, may hold values from -6 to 6
- primary_three: bfloat16 [1024, 512, 512], P(('groups', 'freq')), parts along dimension 0, may hold values from -6 to 6
- window_start: int32 [3, 1024, 512], P(None, ('groups', 'freq')), parts along dimension 1, may hold values from 0 to 255
- window_end: int32 [3, 1024, 512], P(None, ('groups', 'freq')), parts along dimension 1, may hold values from 257 to 512
Outputs:
- predicted: bfloat16 [1024, 512, 512], P(('groups', 'freq')), parts along dimension 0
The draws below stay inside these ranges and needn't reach their ends.
There are 2 independent parts, one for each index of `groups`. The reference program is written for one: setup_inputs(seed, part) draws one part's arguments, and reference() takes and returns one part's arrays. A program takes and returns all parts, laid end to end along the dimension named above; each array names one. Nothing has to cross between parts.
Inputs may be any that keep to these rules, and one draw needn't show every extreme that they name: window_start of a trace is below its window_end.
All inputs are finite; a program needn't handle non-finite values.
Results may differ from the reference program's by a relative error of at most 0.0089.
Values may be sent and summed in bfloat16 or wider, within the bound.
No kernel may reach another device: no remote copies, remote signals or barrier semaphores. Data moves between devices by JAX's collectives and lax.ppermute only.
A program may use at most 64 MiB of HBM per device.

```python
import jax
import jax.numpy as jnp
from jax import lax

NS = 512
NR = 512
NT = 512
NF = 128


def touch_ends(result, stream_key, least, high):
    index_at = [jax.random.randint(jax.random.fold_in(stream_key, axis), (), 0, length) for axis, length in enumerate(result.shape)]
    widest = result.shape.index(max(result.shape))
    beside = index_at[:widest] + [(index_at[widest] + 1) % result.shape[widest]] + index_at[widest + 1:]
    return result.at[tuple(index_at)].set(least).at[tuple(beside)].set(high)


def steps_of(stream_key, shape, cuts, low, largest):
    level = 1.0
    for dim, parts in cuts:
        steps = jax.random.uniform(jax.random.fold_in(jax.random.fold_in(stream_key, 6), dim), (parts,), jnp.float32, low / len(cuts), largest / len(cuts))
        level = level * jnp.repeat(jnp.exp(steps), shape[dim] // parts).reshape((-1,) + (1,) * (len(shape) - 1 - dim))
    return level


def centred(stream_key, shape, spread, reach, pieces=(), kind=jnp.bfloat16):
    gain = steps_of(stream_key, shape, pieces, -0.22, 0.18) if pieces else 1.0
    entries = jax.random.normal(stream_key, shape, jnp.float32) * spread * gain
    return jnp.minimum(jnp.maximum(entries, -reach), reach).astype(kind)


def setup_inputs(seed: int = 0, part: int = 0) -> dict:
    streams_of = jax.random.split(jax.random.key(seed), 6)
    part_splits = jax.random.split(jax.random.fold_in(streams_of[5], part), 6)
    return {
        "primary_one": centred(part_splits[0], (NS, NR, NT), 1.0, 6.0, ((0, 128),)),
        "primary_two": centred(part_splits[1], (NS, NR, NT), 1.0, 6.0, ((0, 128),)),
        "primary_three": centred(part_splits[2], (NS, NR, NT), 1.0, 6.0, ((0, 128),)),
        "window_start": touch_ends(jax.random.randint(part_splits[3], (3, NS, NR), 0, NT // 2), jax.random.fold_in(part_splits[3], 1), 0, (NT // 2) - 1).astype(jnp.int32),
        "window_end": touch_ends(jax.random.randint(part_splits[4], (3, NS, NR), NT // 2 + 1, NT + 1), jax.random.fold_in(part_splits[4], 1), NT // 2 + 1, NT).astype(jnp.int32),
    }


def make_table(count, samples):
    waves = jnp.arange(1, count + 1, dtype=jnp.int32)[:, None]
    times = jnp.arange(samples, dtype=jnp.int32)[None, :]
    phase = waves * times % samples
    angle = 2.0 * jnp.pi / samples * phase.astype(jnp.float32)
    both = jnp.stack([jnp.cos(angle), -jnp.sin(angle)], axis=1)
    return both.reshape(2 * count, samples).astype(jnp.bfloat16)

def spectrum(traces, start, finish, table):
    times = jnp.arange(NT, dtype=jnp.int32)
    inside = (times >= start[:, :, None]) & (times < finish[:, :, None])
    windowed = jnp.where(inside, traces, jnp.zeros_like(traces))
    flat = windowed.reshape(NS * NR, NT)
    spec = lax.dot_general(table, flat, (((1,), (1,)), ((), ())), preferred_element_type=jnp.float32)
    spec = spec * (1.0 / jnp.sqrt(jnp.float32(NT)))
    return spec.astype(jnp.bfloat16).reshape(NF, 2, NS, NR)

def slice_product(items):
    first, second, third = items
    first = first.astype(jnp.float32)
    second = second.astype(jnp.float32)
    third = third.astype(jnp.float32)
    high = lax.Precision.HIGHEST
    cross_re = jnp.dot(first[0], second[0].T, precision=high) + jnp.dot(first[1], second[1].T, precision=high)
    cross_im = jnp.dot(first[1], second[0].T, precision=high) - jnp.dot(first[0], second[1].T, precision=high)
    cross = (jnp.stack([cross_re, cross_im]) * (1.0 / jnp.sqrt(jnp.float32(NR)))).astype(jnp.bfloat16)
    cross = cross.astype(jnp.float32)
    mult_re = jnp.dot(cross[0], third[0], precision=high) - jnp.dot(cross[1], third[1], precision=high)
    mult_im = jnp.dot(cross[0], third[1], precision=high) + jnp.dot(cross[1], third[0], precision=high)
    return (jnp.stack([mult_re, mult_im]) * (1.0 / jnp.sqrt(jnp.float32(NS)))).astype(jnp.bfloat16)

def reference(primary_one, primary_two, primary_three, window_start, window_end):
    table = make_table(NF, NT)
    spec_one = spectrum(primary_one, window_start[0], window_end[0], table)
    spec_two = spectrum(primary_two, window_start[1], window_end[1], table)
    spec_three = spectrum(primary_three, window_start[2], window_end[2], table)
    multiple = lax.map(slice_product, (spec_one, spec_two, spec_three))
    flat = multiple.reshape(2 * NF, NS * NR)
    timed = lax.dot_general(flat, table, (((0,), (0,)), ((), ())), preferred_element_type=jnp.float32)
    timed = timed * (1.0 / jnp.sqrt(jnp.float32(NF)))
    return timed.astype(jnp.bfloat16).reshape(NS, NR, NT)
```

```python
import jax
import jax.numpy as jnp
import numpy as np
from jax import lax
from jax.experimental import pallas as pl
from jax.experimental.pallas import tpu as pltpu
from jax.sharding import PartitionSpec as P

BF = jnp.bfloat16
F32 = jnp.float32
LANE = 128
VMEM_LIMIT = 56 * 1024 * 1024


def make_table(count, samples):
    waves = np.arange(1, count + 1, dtype=np.int64)[:, None]
    times = np.arange(samples, dtype=np.int64)[None, :]
    angle = 2.0 * np.pi / samples * (waves * times % samples)
    both = np.stack([np.cos(angle), -np.sin(angle)], axis=1)
    return both.reshape(2 * count, samples).astype(np.float32)


def swap_matrix(size, half):
    out = np.zeros((size, size), np.float32)
    for base in range(0, size, 2 * half):
        for k in range(half):
            out[base + k, base + half + k] = -1.0
            out[base + half + k, base + k] = 1.0
    return out


def spectra(primaries, window_start, window_end, table):
    sets = len(primaries)
    sources, receivers, samples = primaries[0].shape
    waves = table.shape[0]
    rows = waves * sources
    lanes = receivers // LANE
    scale = 1.0 / float(np.sqrt(samples))

    def body(*refs):
        traces = refs[:sets]
        start_ref, end_ref, table_ref, out_ref, col_ref, acc_ref = refs[sets:]
        step = pl.program_id(0)

        @pl.when(step == 0)
        def _():
            for s in range(sources):
                lines = []
                for j in range(sets):
                    lines.append(start_ref[j, s : s + 1, :])
                    lines.append(end_ref[j, s : s + 1, :])
                lines.append(jnp.zeros((8 - 2 * sets, receivers), jnp.int32))
                col_ref[s] = jnp.transpose(jnp.concatenate(lines, axis=0))

        times = lax.broadcasted_iota(jnp.int32, (receivers, samples), 1)
        cols = col_ref[step]
        for j in range(sets):
            start = cols[:, 2 * j : 2 * j + 1]
            finish = cols[:, 2 * j + 1 : 2 * j + 2]
            inside = (times >= start) & (times < finish)
            x = traces[j][0].astype(F32)
            x = jnp.where(inside, x, 0.0).astype(BF)
            spec = lax.dot_general(
                table_ref[...], x, (((1,), (1,)), ((), ())), preferred_element_type=F32
            )
            spec = spec * scale
            for b in range(lanes):
                acc_ref[j * lanes + b, pl.ds(step, waves, stride=sources), :] = spec[:, b * LANE : (b + 1) * LANE]

        @pl.when(step == sources - 1)
        def _():
            for k in range(sets * lanes):
                out_ref[:, k * LANE : (k + 1) * LANE] = acc_ref[k].astype(BF)

    return pl.pallas_call(
        body,
        grid=(sources,),
        in_specs=[pl.BlockSpec((1, receivers, samples), lambda i: (i, 0, 0))] * sets
        + [
            pl.BlockSpec(window_start.shape, lambda i: (0, 0, 0)),
            pl.BlockSpec(window_end.shape, lambda i: (0, 0, 0)),
            pl.BlockSpec(table.shape, lambda i: (0, 0)),
        ],
        out_specs=pl.BlockSpec((rows, sets * receivers), lambda i: (0, 0)),
        out_shape=jax.ShapeDtypeStruct((rows, sets * receivers), BF),
        scratch_shapes=[
            pltpu.VMEM((sources, receivers, 8), jnp.int32),
            pltpu.VMEM((sets * lanes, rows, LANE), F32),
        ],
        compiler_params=pltpu.CompilerParams(vmem_limit_bytes=VMEM_LIMIT),
        name="spectra",
    )(*primaries, window_start, window_end, table)


def product(received, swap, receivers, sources):
    rows = received.shape[0]
    block = swap.shape[0]
    in_scale = 1.0 / float(np.sqrt(receivers))
    out_scale = 1.0 / float(np.sqrt(sources))

    def turned(x, swap_ref):
        parts = [
            jnp.dot(swap_ref[...], x[k : k + block], preferred_element_type=F32).astype(BF)
            for k in range(0, rows, block)
        ]
        return jnp.concatenate(parts, axis=0)

    def body(x_ref, swap_ref, out_ref, q_re, q_im):
        second = x_ref[:, receivers : 2 * receivers]
        third = x_ref[:, 2 * receivers : 3 * receivers]
        over_rows = (((0,), (0,)), ((), ()))
        re = lax.dot_general(second, third, over_rows, preferred_element_type=F32)
        q_re[...] = (re * in_scale).astype(BF)
        im = lax.dot_general(second, turned(third, swap_ref), over_rows, preferred_element_type=F32)
        q_im[...] = (im * -in_scale).astype(BF)
        first = x_ref[:, :receivers]
        total = jnp.dot(first, q_re[...], preferred_element_type=F32)
        total = total + jnp.dot(turned(first, swap_ref), q_im[...], preferred_element_type=F32)
        out_ref[...] = (total * out_scale).astype(BF)

    return pl.pallas_call(
        body,
        out_shape=jax.ShapeDtypeStruct((rows, receivers), BF),
        scratch_shapes=[pltpu.VMEM((receivers, receivers), BF)] * 2,
        compiler_params=pltpu.CompilerParams(vmem_limit_bytes=VMEM_LIMIT),
        name="product",
    )(received, swap)


def inverse(returned, table, sources):
    rows, receivers = returned.shape
    waves, samples = table.shape
    lanes = receivers // LANE
    scale = 1.0 / float(np.sqrt(waves // 2))

    def body(x_ref, table_ref, out_ref, wide_ref):
        step = pl.program_id(0)

        @pl.when(step == 0)
        def _():
            for b in range(lanes):
                wide_ref[b] = x_ref[:, b * LANE : (b + 1) * LANE].astype(F32)

        parts = [wide_ref[b, pl.ds(step, waves, stride=sources), :].astype(BF) for b in range(lanes)]
        x = jnp.concatenate(parts, axis=1)
        timed = lax.dot_general(x, table_ref[...], (((0,), (0,)), ((), ())), preferred_element_type=F32)
        out_ref[0] = (timed * scale).astype(BF)

    return pl.pallas_call(
        body,
        grid=(sources,),
        in_specs=[
            pl.BlockSpec((rows, receivers), lambda i: (0, 0)),
            pl.BlockSpec((waves, samples), lambda i: (0, 0)),
        ],
        out_specs=pl.BlockSpec((1, receivers, samples), lambda i: (i, 0, 0)),
        out_shape=jax.ShapeDtypeStruct((sources, receivers, samples), BF),
        scratch_shapes=[pltpu.VMEM((lanes, rows, LANE), F32)],
        compiler_params=pltpu.CompilerParams(vmem_limit_bytes=VMEM_LIMIT),
        name="inverse",
    )(returned, table)


def on_device(primary_one, primary_two, primary_three, window_start, window_end):
    sources, receivers, samples = primary_one.shape
    count = lax.axis_size("freq")
    table = jnp.asarray(make_table(count, samples), BF)
    swap = jnp.asarray(swap_matrix(256, sources), BF)
    sent = spectra((primary_one, primary_two, primary_three), window_start, window_end, table)
    received = lax.all_to_all(sent, "freq", split_axis=0, concat_axis=0, tiled=True)
    multiple = product(received, swap, receivers, sources * count)
    returned = lax.all_to_all(multiple, "freq", split_axis=0, concat_axis=0, tiled=True)
    return inverse(returned, table, sources)


def solution(mesh):
    split = P(("groups", "freq"), None, None)
    windows = P(None, ("groups", "freq"), None)
    return jax.shard_map(
        on_device,
        mesh=mesh,
        in_specs=(split, split, split, windows, windows),
        out_specs=split,
        check_vma=False,
    )
```

```python
import jax
import jax.numpy as jnp
import numpy as np
from jax import lax
from jax.experimental import pallas as pl
from jax.experimental.pallas import tpu as pltpu
from jax.sharding import PartitionSpec as P

BF = jnp.bfloat16
F32 = jnp.float32
LANE = 128
VMEM_LIMIT = 56 * 1024 * 1024


def make_table(count, samples):
    waves = np.arange(1, count + 1, dtype=np.int64)[:, None]
    times = np.arange(samples, dtype=np.int64)[None, :]
    angle = 2.0 * np.pi / samples * (waves * times % samples)
    both = np.stack([np.cos(angle), -np.sin(angle)], axis=1)
    return both.reshape(2 * count, samples).astype(np.float32)


def swap_matrix(size, half):
    out = np.zeros((size, size), np.float32)
    for base in range(0, size, 2 * half):
        for k in range(half):
            out[base + k, base + half + k] = -1.0
            out[base + half + k, base + k] = 1.0
    return out


def spectra(primaries, window_start, window_end, table):
    sets = len(primaries)
    sources, receivers, samples = primaries[0].shape
    waves = table.shape[0]
    rows = waves * sources
    lanes = receivers // LANE
    half = samples // 2
    scale = 1.0 / float(np.sqrt(samples))

    def body(*refs):
        traces = refs[:sets]
        start_ref, end_ref, table_ref, out_ref, buf_ref, col_ref, acc_ref, sems = refs[sets:]

        def fetch(j, s):
            return pltpu.make_async_copy(traces[j].at[s], buf_ref.at[j, s], sems.at[j, s])

        for j in range(sets):
            for s in range(sources):
                fetch(j, s).start()
        for s in range(sources):
            lines = []
            for j in range(sets):
                lines.append(start_ref[j, s : s + 1, :])
                lines.append(end_ref[j, s : s + 1, :] - half)
            lines.append(jnp.zeros((8 - 2 * sets, receivers), jnp.int32))
            col_ref[s] = jnp.transpose(jnp.concatenate(lines, axis=0).astype(F32))

        times = lax.broadcasted_iota(jnp.int32, (receivers, half), 1).astype(F32).astype(BF)
        zero = jnp.zeros((receivers, half), BF)

        def one(s, j):
            fetch(j, s).wait()
            cols = col_ref[s]
            start = jnp.broadcast_to(cols[:, 2 * j : 2 * j + 1], (receivers, half)).astype(BF)
            finish = jnp.broadcast_to(cols[:, 2 * j + 1 : 2 * j + 2], (receivers, half)).astype(BF)
            early = jnp.where(times >= start, buf_ref[j, s, :, :half], zero)
            late = jnp.where(times < finish, buf_ref[j, s, :, half:], zero)
            across = (((1,), (1,)), ((), ()))
            kept = jnp.concatenate([early, late], axis=1)
            spec = lax.dot_general(table_ref[...], kept, across, preferred_element_type=F32)
            for b in range(lanes):
                acc_ref[b, pl.ds(s, waves, stride=sources), :] = spec[:, b * LANE : (b + 1) * LANE] * scale

        for j in range(sets):
            @pl.loop(0, sources)
            def _(s):
                one(s, j)
            for b in range(lanes):
                at = j * receivers + b * LANE
                out_ref[:, at : at + LANE] = acc_ref[b].astype(BF)

    vmem = pl.BlockSpec(memory_space=pltpu.VMEM)
    return pl.pallas_call(
        body,
        in_specs=[pl.BlockSpec(memory_space=pl.ANY)] * sets + [vmem] * 3,
        out_specs=vmem,
        out_shape=pltpu.VMEM((rows, sets * receivers), BF),
        scratch_shapes=[
            pltpu.VMEM((sets, sources, receivers, samples), BF),
            pltpu.VMEM((sources, receivers, 8), F32),
            pltpu.VMEM((lanes, rows, LANE), F32),
            pltpu.SemaphoreType.DMA((sets, sources)),
        ],
        compiler_params=pltpu.CompilerParams(vmem_limit_bytes=VMEM_LIMIT),
        name="spectra",
    )(*primaries, window_start, window_end, table)


def product(received, swap, receivers, sources):
    rows = received.shape[0]
    block = swap.shape[0]
    in_scale = 1.0 / float(np.sqrt(receivers))
    out_scale = 1.0 / float(np.sqrt(sources))

    def turned(x, swap_ref):
        parts = [
            jnp.dot(swap_ref[...], x[k : k + block], preferred_element_type=F32).astype(BF)
            for k in range(0, rows, block)
        ]
        return jnp.concatenate(parts, axis=0)

    def body(x_ref, swap_ref, out_ref, q_re, q_im):
        second = x_ref[:, receivers : 2 * receivers]
        third = x_ref[:, 2 * receivers : 3 * receivers]
        over_rows = (((0,), (0,)), ((), ()))
        re = lax.dot_general(second, third, over_rows, preferred_element_type=F32)
        q_re[...] = (re * in_scale).astype(BF)
        im = lax.dot_general(second, turned(third, swap_ref), over_rows, preferred_element_type=F32)
        q_im[...] = (im * -in_scale).astype(BF)
        first = x_ref[:, :receivers]
        total = jnp.dot(first, q_re[...], preferred_element_type=F32)
        total = total + jnp.dot(turned(first, swap_ref), q_im[...], preferred_element_type=F32)
        out_ref[...] = (total * out_scale).astype(BF)

    vmem = pl.BlockSpec(memory_space=pltpu.VMEM)
    return pl.pallas_call(
        body,
        in_specs=[vmem, vmem],
        out_specs=vmem,
        out_shape=pltpu.VMEM((rows, receivers), BF),
        scratch_shapes=[pltpu.VMEM((receivers, receivers), BF)] * 2,
        compiler_params=pltpu.CompilerParams(vmem_limit_bytes=VMEM_LIMIT),
        name="product",
    )(received, swap)


def inverse(returned, table, sources):
    rows, receivers = returned.shape
    waves, samples = table.shape
    lanes = receivers // LANE
    scale = 1.0 / float(np.sqrt(waves // 2))

    def body(x_ref, table_ref, out_ref, wide_ref, timed_ref, sems):
        for b in range(lanes):
            wide_ref[b] = x_ref[:, b * LANE : (b + 1) * LANE].astype(F32)
        copies = []
        for s in range(sources):
            parts = [wide_ref[b, pl.ds(s, waves, stride=sources), :].astype(BF) for b in range(lanes)]
            x = jnp.concatenate(parts, axis=1)
            timed = lax.dot_general(x, table_ref[...], (((0,), (0,)), ((), ())), preferred_element_type=F32)
            timed_ref[s] = (timed * scale).astype(BF)
            copy = pltpu.make_async_copy(timed_ref.at[s], out_ref.at[s], sems.at[s])
            copy.start()
            copies.append(copy)
        for copy in copies:
            copy.wait()

    vmem = pl.BlockSpec(memory_space=pltpu.VMEM)
    return pl.pallas_call(
        body,
        in_specs=[vmem, vmem],
        out_specs=pl.BlockSpec(memory_space=pl.ANY),
        out_shape=jax.ShapeDtypeStruct((sources, receivers, samples), BF),
        scratch_shapes=[
            pltpu.VMEM((lanes, rows, LANE), F32),
            pltpu.VMEM((sources, receivers, samples), BF),
            pltpu.SemaphoreType.DMA((sources,)),
        ],
        compiler_params=pltpu.CompilerParams(vmem_limit_bytes=VMEM_LIMIT),
        name="inverse",
    )(returned, table)


def on_device(primary_one, primary_two, primary_three, window_start, window_end):
    sources, receivers, samples = primary_one.shape
    count = lax.axis_size("freq")
    table = jnp.asarray(make_table(count, samples), BF)
    swap = jnp.asarray(swap_matrix(256, sources), BF)
    sent = spectra((primary_one, primary_two, primary_three), window_start, window_end, table)
    received = lax.all_to_all(sent, "freq", split_axis=0, concat_axis=0, tiled=True)
    received = pltpu.with_memory_space_constraint(received, pltpu.VMEM)
    multiple = product(received, swap, receivers, sources * count)
    returned = lax.all_to_all(multiple, "freq", split_axis=0, concat_axis=0, tiled=True)
    returned = pltpu.with_memory_space_constraint(returned, pltpu.VMEM)
    return inverse(returned, table, sources)


def solution(mesh):
    split = P(("groups", "freq"), None, None)
    windows = P(None, ("groups", "freq"), None)
    return jax.shard_map(
        on_device,
        mesh=mesh,
        in_specs=(split, split, split, windows, windows),
        out_specs=split,
        check_vma=False,
    )
```
